32 devices in a mesh: band: 8 (over z, y), grid: 4 (over x, core).
Axes of the slice: x: 2, y: 2, z: 4, core: 2. Of those that a mesh axis runs over, the one named last changes fastest.
Arguments:
- orbitals: float32 [24, 64, 4096], P('band', 'grid'), may hold values from -6 to 6
- pair_mask: int32 [24, 24], replicated, may hold values from 0 to 1, as said below
Outputs:
- exchange_term: float32 [24, 64, 4096], P('band', 'grid')
The draws below stay inside these ranges and needn't reach their ends.
Inputs may be any that keep to these rules, and one draw needn't show every extreme that they name: pair_mask is symmetric; entries outside the candidate pairs of every block (and their transposes) are 0; each block has at most 12 candidate pairs with mask 1, and some block has exactly 12.
All inputs are finite; a program needn't handle non-finite values.
Results may differ from the reference program's by a relative error of at most 0.00027.
Values sent between devices are 32-bit elements; how exact they have to be, the bound alone decides.
No kernel may reach another device: no remote copies, remote signals or barrier semaphores. Data moves between devices by JAX's collectives and lax.ppermute only.
A program may use at most 64 MiB of HBM per device.

```python
import math
import jax
import jax.numpy as jnp
import numpy as np
from jax import lax

NG = 64
ORB_DEV = 3
REACH = 2
NORB = 24
NCAND = 24
CAP = 12


def pair_table_drawn():
    entries = []
    for distance in range(REACH + 1):
        for leading_orbital in range(ORB_DEV):
            for second_orb in range(ORB_DEV):
                if distance > 0 or leading_orbital <= second_orb:
                    entries.append((leading_orbital, distance, second_orb))
    return np.array(entries, dtype=np.int32)


def draw_orbitals(key, part):
    full_shape = (NORB, NG, NG * NG)
    values_out = jax.random.normal(key, full_shape, jnp.float32)
    return jnp.clip(values_out, -6.0, 6.0)


def draw_pair_mask(key, part):
    pair_list = pair_table_drawn()
    groups = NORB // ORB_DEV
    key_counts, key_full, key_scores = jax.random.split(jax.random.fold_in(key, 17), 3)
    counts = jax.random.randint(key_counts, (groups,), 1, CAP + 1)
    full_group = jax.random.randint(key_full, (), 0, groups)
    counts = jnp.where(jnp.arange(groups, dtype=jnp.int32) == full_group, CAP, counts)
    scores = jax.random.randint(key_scores, (groups, NCAND), 0, 1 << 20) * NCAND + jnp.arange(NCAND, dtype=jnp.int32)[None, :]
    ranks = jnp.argsort(jnp.argsort(scores, axis=1), axis=1)
    live_flags = (ranks < counts[:, None]).astype(jnp.int32)
    group_ids = jnp.arange(groups, dtype=jnp.int32)[:, None]
    row_ids = group_ids * ORB_DEV + jnp.asarray(pair_list[:, 0])[None, :]
    col_ids = (group_ids + jnp.asarray(pair_list[:, 1])[None, :]) % groups * ORB_DEV + jnp.asarray(pair_list[:, 2])[None, :]
    mask_out = jnp.zeros((NORB, NORB), jnp.int32)
    mask_out = mask_out.at[row_ids.reshape(-1), col_ids.reshape(-1)].set(live_flags.reshape(-1))
    mask_out = mask_out.at[col_ids.reshape(-1), row_ids.reshape(-1)].set(live_flags.reshape(-1))
    return mask_out


def setup_inputs(seed: int = 0) -> dict:
    key_list = jax.random.split(jax.random.key(seed), 3)
    return {
        "orbitals": draw_orbitals(jax.random.fold_in(key_list[2], 71), 0),
        "pair_mask": draw_pair_mask(jax.random.fold_in(key_list[2], 71), 0),
    }


MIXING = 0.25
BOX_LENGTH = 16.0


def pair_table():
    entries = []
    for distance in range(REACH + 1):
        for leading_orbital in range(ORB_DEV):
            for second_orb in range(ORB_DEV):
                if distance > 0 or leading_orbital <= second_orb:
                    entries.append((leading_orbital, distance, second_orb))
    return np.array(entries, dtype=np.int32)


def poisson_green_kernel():
    positions = jnp.arange(NG, dtype=jnp.int32)
    signed_waves = jnp.where(positions < NG // 2, positions, positions - NG)
    squared = (signed_waves[:, None, None] ** 2 + signed_waves[None, :, None] ** 2
               + signed_waves[None, None, :] ** 2)
    safe_values = jnp.maximum(squared, 1).astype(jnp.float32)
    return jnp.where(squared > 0, jnp.float32(BOX_LENGTH * BOX_LENGTH / math.pi) / safe_values,
                     jnp.float32(0.0))


def reference(orbitals, pair_mask):
    groups = NORB // ORB_DEV
    pair_list = pair_table()
    band_ids = np.arange(groups, dtype=np.int32)[:, None]
    row_ids = (band_ids * ORB_DEV + pair_list[None, :, 0]).reshape(-1).astype(np.int32)
    col_ids = (((band_ids + pair_list[None, :, 1]) % groups) * ORB_DEV
               + pair_list[None, :, 2]).reshape(-1).astype(np.int32)
    weights = pair_mask[jnp.asarray(row_ids), jnp.asarray(col_ids)].astype(jnp.float32)
    cross_flags = jnp.asarray((row_ids != col_ids).astype(np.float32)).astype(jnp.float32)
    cubes = orbitals.reshape(NORB, NG, NG, NG)
    kernel = poisson_green_kernel()

    def one_pair(totals, pair_input):
        row_id, col_id, weight, cross_flag = pair_input
        first_cube = cubes[row_id]
        second_cube = cubes[col_id]
        potential = jnp.real(jnp.fft.ifftn(jnp.fft.fftn(first_cube * second_cube) * kernel))
        totals = totals.at[row_id].add(weight * potential * second_cube)
        totals = totals.at[col_id].add(weight * cross_flag * potential * first_cube)
        return totals, None

    totals, discarded_value = lax.scan(one_pair, jnp.zeros((NORB, NG, NG, NG), jnp.float32),
                              (jnp.asarray(row_ids).astype(jnp.int32), jnp.asarray(col_ids).astype(jnp.int32),
                               weights, cross_flags))
    return (-MIXING * totals).reshape(NORB, NG, NG * NG)
```

```python
import math

import jax
import jax.numpy as jnp
import numpy as np
from jax import lax
from jax.experimental import pallas as pl
from jax.experimental.pallas import tpu as pltpu
from jax.sharding import PartitionSpec as P

ORB_DEV = 3
REACH = 2
CAP = 12
MIXING = 0.25
BOX_LENGTH = 16.0
GROUP = 4
BLOCK_PLANES = 8


def shifted(block, axis, distance):
    count = lax.axis_size(axis)
    return lax.ppermute(block, axis, [((i - distance) % count, i) for i in range(count)])


def pair_table():
    entries = []
    for distance in range(REACH + 1):
        for leading in range(ORB_DEV):
            for second in range(ORB_DEV):
                if distance > 0 or leading <= second:
                    entries.append((leading, distance, second))
    return np.array(entries, dtype=np.int32)


def split_table(table):
    high = table.astype(np.float32).astype(jnp.bfloat16)
    low = (table - high.astype(np.float64)).astype(np.float32).astype(jnp.bfloat16)
    return jnp.asarray(high), jnp.asarray(low)


def dft_tables(n):
    k = np.arange(n)
    angles = (k[:, None] * k[None, :] % n) * (2.0 * math.pi / n)
    c, s = np.cos(angles), np.sin(angles)
    forward = np.array([[c, -s], [s, c]])
    inverse = np.array([[c, s], [-s, c]])
    e = np.eye(2)
    z_forward = np.einsum("cdzk,qr,yw->cqyzdwrk", forward, e, e).reshape(8 * n, 8 * n)
    z_inverse = np.einsum("cdkz,qr,yw->cyqkdrwz", inverse, e, e).reshape(8 * n, 8 * n)
    f4 = forward.reshape(2, 2, n // 2, 2, n)
    y_forward = f4.transpose(1, 4, 0, 3, 2).reshape(2 * n, 2 * n)
    i4 = inverse.reshape(2, 2, n, n // 2, 2)
    y_inverse = i4.transpose(1, 4, 3, 0, 2).reshape(2 * n, 2 * n)
    x_forward = forward.transpose(1, 3, 0, 2).reshape(2 * n, 2 * n)
    x_inverse = inverse.transpose(1, 3, 0, 2).reshape(2 * n, 2 * n)
    named = (z_forward, y_forward, x_forward, x_inverse, y_inverse, z_inverse)
    return [split_table(t) for t in named]


def dot(a, b):
    return jnp.dot(a, b, preferred_element_type=jnp.float32)


def halves(x):
    high = x.astype(jnp.bfloat16)
    return high, (x - high.astype(jnp.float32)).astype(jnp.bfloat16)


def left(th, tl, x):
    xh, xl = halves(x)
    return dot(th[...], xh) + (dot(tl[...], xh) + dot(th[...], xl))


def right(x, th, tl):
    xh, xl = halves(x)
    return dot(xh, th[...]) + (dot(xh, tl[...]) + dot(xl, th[...]))


def whole_spec(table):
    return pl.BlockSpec(table.shape, lambda *_: (0,) * table.ndim)


def orbital_specs(group, bx, rows, lanes):
    def spec(which, p):
        return pl.BlockSpec(
            (1, bx, rows, lanes), lambda i, *s: (s[which][group * GROUP + p], i, 0, 0)
        )

    return [spec(0, p) for p in range(GROUP)] + [spec(1, p) for p in range(GROUP)]


def forward_planes(group, scalars, flat, tables, parts):
    _, planes, rows, lanes = flat.shape
    n = lanes // 2
    width = n // parts
    bx = BLOCK_PLANES

    def body(*refs):
        refs = refs[len(scalars):]
        leads, seconds = refs[:GROUP], refs[GROUP : 2 * GROUP]
        zh, zl, yh, yl, out = refs[2 * GROUP :]
        rho = [(a[0] * b[0]).reshape(bx * rows, lanes) for a, b in zip(leads, seconds)]
        z = right(jnp.concatenate(rho, axis=1), zh, zl)
        cols = [
            jnp.concatenate(
                [z[x * rows : (x + 1) * rows, i * lanes : (i + 1) * lanes] for i in range(4)],
                axis=0,
            )
            for x in range(bx)
        ]
        y = left(yh, yl, jnp.concatenate(cols, axis=1))
        stacked = jnp.stack([y[:, x * lanes : (x + 1) * lanes] for x in range(bx)], axis=0)
        turned = jnp.swapaxes(stacked, 0, 1)
        for d in range(parts):
            for c in range(2):
                start = c * n + d * width
                out[d, c] = turned[start : start + width]

    ops = [*tables[0], *tables[1]]
    return pl.pallas_call(
        body,
        grid_spec=pltpu.PrefetchScalarGridSpec(
            num_scalar_prefetch=len(scalars),
            grid=(planes // bx,),
            in_specs=orbital_specs(group, bx, rows, lanes) + [whole_spec(t) for t in ops],
            out_specs=pl.BlockSpec((parts, 2, width, bx, lanes), lambda i, *_: (0, 0, 0, i, 0)),
        ),
        out_shape=jax.ShapeDtypeStruct((parts, 2, width, planes, lanes), jnp.float32),
        name=f"forward_planes_{group}",
    )(*scalars, *([flat] * (2 * GROUP)), *ops)


def solve_columns(group, columns, kernel, tables):
    parts, _, width, planes, lanes = columns.shape
    n = parts * planes
    bk = BLOCK_PLANES

    def body(data, kern, fh, fl, ih, il, out):
        cols = []
        for k in range(bk):
            pieces = [data[d, c, k] for c in range(2) for d in range(parts)]
            cols.append(jnp.concatenate(pieces, axis=0))
        spectrum = left(fh, fl, jnp.concatenate(cols, axis=1))
        weights = jnp.concatenate([kern[k] for k in range(bk)], axis=1)
        spectrum = spectrum * jnp.concatenate([weights, weights], axis=0)
        back = left(ih, il, spectrum)
        for k in range(bk):
            for c in range(2):
                for d in range(parts):
                    start = c * n + d * planes
                    out[d, c, k] = back[start : start + planes, k * lanes : (k + 1) * lanes]

    ops = [*tables[2], *tables[3]]
    block = pl.BlockSpec((parts, 2, bk, planes, lanes), lambda i: (0, 0, i, 0, 0))
    return pl.pallas_call(
        body,
        grid=(width // bk,),
        in_specs=[block, pl.BlockSpec((bk, n, lanes), lambda i: (i, 0, 0))]
        + [whole_spec(t) for t in ops],
        out_specs=block,
        out_shape=jax.ShapeDtypeStruct(columns.shape, jnp.float32),
        name=f"solve_columns_{group}",
    )(columns, kernel, *ops)


def add_exchange(group, scalars, returned, flat, totals, tables):
    slots, planes, rows, lanes = flat.shape
    parts, _, width, _, _ = returned.shape
    bx = BLOCK_PLANES

    def body(*refs):
        first, slot, weight, cross = refs[: len(scalars)]
        refs = refs[len(scalars):]
        data = refs[0]
        leads, seconds = refs[1 : 1 + GROUP], refs[1 + GROUP : 1 + 2 * GROUP]
        yh, yl, zh, zl = refs[1 + 2 * GROUP : 5 + 2 * GROUP]
        out = refs[-1]
        pieces = [data[d, c] for c in range(2) for d in range(parts)]
        turned = jnp.swapaxes(jnp.concatenate(pieces, axis=0), 0, 1)
        y = left(yh, yl, jnp.concatenate([turned[x] for x in range(bx)], axis=1))
        lines = [
            jnp.concatenate(
                [y[i * rows : (i + 1) * rows, x * lanes : (x + 1) * lanes] for i in range(4)],
                axis=1,
            )
            for x in range(bx)
        ]
        v = right(jnp.concatenate(lines, axis=0), zh, zl)
        if totals is None:
            out[...] = jnp.zeros_like(out)
        else:
            out[...] = refs[-2][...]
        for p in range(GROUP):
            at = group * GROUP + p
            potential = v[:, p * lanes : (p + 1) * lanes].reshape(bx, rows, lanes)
            out[first[at]] += weight[at] * potential * seconds[p][0]
            out[slot[at]] += cross[at] * potential * leads[p][0]

    ops = [*tables[4], *tables[5]]
    total_spec = pl.BlockSpec((slots, bx, rows, lanes), lambda i, *_: (0, i, 0, 0))
    in_specs = [pl.BlockSpec((parts, 2, width, bx, lanes), lambda i, *_: (0, 0, 0, i, 0))]
    in_specs += orbital_specs(group, bx, rows, lanes) + [whole_spec(t) for t in ops]
    args = [*scalars, returned, *([flat] * (2 * GROUP)), *ops]
    aliases = {}
    if totals is not None:
        in_specs.append(total_spec)
        aliases = {len(args): 0}
        args.append(totals)
    return pl.pallas_call(
        body,
        grid_spec=pltpu.PrefetchScalarGridSpec(
            num_scalar_prefetch=len(scalars),
            grid=(planes // bx,),
            in_specs=in_specs,
            out_specs=total_spec,
        ),
        out_shape=jax.ShapeDtypeStruct(flat.shape, jnp.float32),
        input_output_aliases=aliases,
        name=f"add_exchange_{group}",
    )(*args)


def live_pairs(pair_mask):
    pairs = pair_table()
    count = pairs.shape[0]
    slots = -(-CAP // GROUP) * GROUP
    band = lax.axis_index("band")
    groups = lax.axis_size("band")
    rows = band * ORB_DEV + jnp.asarray(pairs[:, 0])
    cols = (band + jnp.asarray(pairs[:, 1])) % groups * ORB_DEV + jnp.asarray(pairs[:, 2])
    live = pair_mask[rows, cols]
    earlier = np.tril(np.ones((count, count), np.int32), -1)
    rank = jnp.sum(jnp.asarray(earlier) * live[None, :], axis=1)
    hot = (rank[None, :] == jnp.arange(slots, dtype=jnp.int32)[:, None]) * live[None, :]
    slot_of = pairs[:, 1] * ORB_DEV + pairs[:, 2]
    cross_of = (slot_of != pairs[:, 0]).astype(np.int32)
    first = jnp.sum(hot * jnp.asarray(pairs[:, 0])[None, :], axis=1)
    slot = jnp.sum(hot * jnp.asarray(slot_of.astype(np.int32))[None, :], axis=1)
    weight = jnp.sum(hot, axis=1).astype(jnp.float32)
    cross = jnp.sum(hot * jnp.asarray(cross_of)[None, :], axis=1).astype(jnp.float32)
    return first, slot, weight, cross


def green_kernel(n, width):
    def wave(positions):
        return jnp.where(positions < n // 2, positions, positions - n)

    ky = wave(lax.axis_index("grid") * width + jnp.arange(width, dtype=jnp.int32))
    k = wave(jnp.arange(n, dtype=jnp.int32))
    kz = wave(jnp.arange(2 * n, dtype=jnp.int32) % n)
    squared = (ky * ky)[:, None, None] + (k * k)[None, :, None] + (kz * kz)[None, None, :]
    safe = jnp.maximum(squared, 1).astype(jnp.float32)
    scale = BOX_LENGTH * BOX_LENGTH / math.pi / float(n**3)
    return jnp.where(squared > 0, scale / safe, 0.0)


def local(orbitals, pair_mask):
    orb_count, planes, cells = orbitals.shape
    n = math.isqrt(cells)
    parts = lax.axis_size("grid")
    tables = dft_tables(n)
    own = orbitals.reshape(orb_count, planes, n // 2, 2 * n)
    visits = [own] + [shifted(own, "band", -d) for d in range(1, REACH + 1)]
    flat = jnp.concatenate(visits, axis=0)
    scalars = live_pairs(pair_mask)
    kernel = green_kernel(n, n // parts)

    def exchange(block):
        return lax.all_to_all(block, "grid", split_axis=0, concat_axis=0, tiled=True)

    turns = range(-(-CAP // GROUP))
    spectra = [forward_planes(g, scalars[:2], flat, tables, parts) for g in turns]
    columns = [exchange(s) for s in spectra]
    solved = [solve_columns(g, columns[g], kernel, tables) for g in turns]
    returned = [exchange(s) for s in solved]
    totals = None
    for g in turns:
        totals = add_exchange(g, scalars, returned[g], flat, totals, tables)
    owned = totals[:orb_count]
    for d in range(1, REACH + 1):
        owned = owned + shifted(totals[d * orb_count : (d + 1) * orb_count], "band", d)
    return (-MIXING * owned).reshape(orb_count, planes, cells)


def solution(mesh):
    return jax.shard_map(
        local,
        mesh=mesh,
        in_specs=(P("band", "grid", None), P()),
        out_specs=P("band", "grid", None),
        check_vma=False,
    )
```

```python
import math

import jax
import jax.numpy as jnp
import numpy as np
from jax import lax
from jax.experimental import pallas as pl
from jax.experimental.pallas import tpu as pltpu
from jax.sharding import PartitionSpec as P

ORB_DEV = 3
REACH = 2
CAP = 12
MIXING = 0.25
BOX_LENGTH = 16.0
GROUP = 4
BLOCK_PLANES = 8


def shifted(block, axis, distance):
    count = lax.axis_size(axis)
    return lax.ppermute(block, axis, [((i - distance) % count, i) for i in range(count)])


def pair_table():
    entries = []
    for distance in range(REACH + 1):
        for leading in range(ORB_DEV):
            for second in range(ORB_DEV):
                if distance > 0 or leading <= second:
                    entries.append((leading, distance, second))
    return np.array(entries, dtype=np.int32)


def split_table(table):
    high = table.astype(np.float32).astype(jnp.bfloat16)
    low = (table - high.astype(np.float64)).astype(np.float32).astype(jnp.bfloat16)
    return jnp.asarray(high), jnp.asarray(low)


def peer_order(parts):
    power = parts & (parts - 1) == 0
    return [[m ^ s if power else (m + s) % parts for s in range(parts)] for m in range(parts)]


def block_order(table, parts, side):
    n = table.shape[0] // 2
    stacked = []
    for order in peer_order(parts):
        index = np.arange(2 * n).reshape(2, parts, n // parts)[:, order].reshape(-1)
        stacked.append(table[index] if side == 0 else table[:, index])
    return np.stack(stacked)


def dft_tables(n, parts):
    k = np.arange(n)
    angles = (k[:, None] * k[None, :] % n) * (2.0 * math.pi / n)
    c, s = np.cos(angles), np.sin(angles)
    forward = np.array([[c, -s], [s, c]])
    inverse = np.array([[c, s], [-s, c]])
    e = np.eye(2)
    z_forward = np.einsum("cdzk,qr,yw->cqyzdwrk", forward, e, e).reshape(8 * n, 8 * n)
    f4 = forward.reshape(2, 2, n // 2, 2, n)
    y_forward = f4.transpose(1, 4, 0, 3, 2).reshape(2 * n, 2 * n)
    i4 = inverse.reshape(2, 2, n, n // 2, 2)
    y_inverse = i4.transpose(1, 4, 3, 0, 2).reshape(2 * n, 2 * n)
    x_forward = forward.transpose(1, 3, 0, 2).reshape(2 * n, 2 * n)
    x_inverse = inverse.transpose(1, 3, 0, 2).reshape(2 * n, 2 * n)
    y_forward = block_order(y_forward, parts, 0)
    x_forward = block_order(x_forward, parts, 1)
    x_inverse = block_order(x_inverse, parts, 0)
    y_inverse = block_order(y_inverse, parts, 1)
    named = (z_forward, y_forward, x_forward, x_inverse, y_inverse)
    return [split_table(t) for t in named]


def dot(a, b):
    return jnp.dot(a, b, preferred_element_type=jnp.float32)


def halves(x):
    high = x.astype(jnp.bfloat16)
    return high, (x - high.astype(jnp.float32)).astype(jnp.bfloat16)


def left(th, tl, x):
    xh, xl = halves(x)
    return dot(th[...], xh) + (dot(tl[...], xh) + dot(th[...], xl))


def right(x, th, tl):
    xh, xl = halves(x)
    return dot(xh, th[...]) + (dot(xh, tl[...]) + dot(xl, th[...]))


def right_transposed(x, th, tl):
    def dot_t(a, b):
        return lax.dot_general(a, b, (((1,), (1,)), ((), ())), preferred_element_type=jnp.float32)

    xh, xl = halves(x)
    return dot_t(xh, th[...]) + (dot_t(xh, tl[...]) + dot_t(xl, th[...]))


def table_spec(table):
    if table.ndim == 2:
        return pl.BlockSpec(table.shape, lambda *_: (0, 0))
    return pl.BlockSpec((pl.squeezed, *table.shape[1:]), lambda i, me, *_: (me[0], 0, 0))


def orbital_specs(group, bx, rows, lanes):
    def spec(which, p):
        return pl.BlockSpec(
            (1, bx, rows, lanes), lambda i, *s: (s[which + 1][group * GROUP + p], i, 0, 0)
        )

    return [spec(0, p) for p in range(GROUP)] + [spec(1, p) for p in range(GROUP)]


def forward_planes(group, scalars, flat, tables, parts):
    _, planes, rows, lanes = flat.shape
    n = lanes // 2
    width = n // parts
    bx = BLOCK_PLANES

    def body(*refs):
        refs = refs[len(scalars):]
        leads, seconds = refs[:GROUP], refs[GROUP : 2 * GROUP]
        zh, zl, yh, yl = refs[2 * GROUP : 2 * GROUP + 4]
        outs = refs[2 * GROUP + 4 :]
        rho = [(a[0] * b[0]).reshape(bx * rows, lanes) for a, b in zip(leads, seconds)]
        z = right(jnp.concatenate(rho, axis=1), zh, zl)
        cols = [
            jnp.concatenate(
                [z[x * rows : (x + 1) * rows, i * lanes : (i + 1) * lanes] for i in range(4)],
                axis=0,
            )
            for x in range(bx)
        ]
        y = left(yh, yl, jnp.concatenate(cols, axis=1))
        stacked = jnp.stack([y[:, x * lanes : (x + 1) * lanes] for x in range(bx)], axis=0)
        turned = jnp.swapaxes(stacked, 0, 1)
        for d in range(parts):
            for c in range(2):
                start = c * n + d * width
                outs[d][c] = turned[start : start + width]

    ops = [*tables[0], *tables[1]]
    return pl.pallas_call(
        body,
        grid_spec=pltpu.PrefetchScalarGridSpec(
            num_scalar_prefetch=len(scalars),
            grid=(planes // bx,),
            in_specs=orbital_specs(group, bx, rows, lanes) + [table_spec(t) for t in ops],
            out_specs=[pl.BlockSpec((2, width, bx, lanes), lambda i, *_: (0, 0, i, 0))] * parts,
        ),
        out_shape=[jax.ShapeDtypeStruct((2, width, planes, lanes), jnp.float32)] * parts,
        name=f"forward_planes_{group}",
    )(*scalars, *([flat] * (2 * GROUP)), *ops)


def solve_columns(group, me, columns, kernel, tables):
    parts = len(columns)
    _, width, planes, lanes = columns[0].shape
    n = parts * planes
    bk = BLOCK_PLANES

    def body(_, *refs):
        data, outs = refs[:parts], refs[parts + 5 :]
        kern, fh, fl, ih, il = refs[parts : parts + 5]
        cols = []
        for k in range(bk):
            pieces = [data[d][c, k] for c in range(2) for d in range(parts)]
            cols.append(jnp.concatenate(pieces, axis=0))
        spectrum = left(fh, fl, jnp.concatenate(cols, axis=1))
        weights = jnp.concatenate([kern[k] for k in range(bk)], axis=1)
        spectrum = spectrum * jnp.concatenate([weights, weights], axis=0)
        back = left(ih, il, spectrum)
        for k in range(bk):
            for c in range(2):
                for d in range(parts):
                    start = c * n + d * planes
                    outs[d][c, k] = back[start : start + planes, k * lanes : (k + 1) * lanes]

    ops = [*tables[2], *tables[3]]
    block = pl.BlockSpec((2, bk, planes, lanes), lambda i, *_: (0, i, 0, 0))
    return pl.pallas_call(
        body,
        grid_spec=pltpu.PrefetchScalarGridSpec(
            num_scalar_prefetch=1,
            grid=(width // bk,),
            in_specs=[block] * parts
            + [pl.BlockSpec((bk, n, lanes), lambda i, *_: (i, 0, 0))]
            + [table_spec(t) for t in ops],
            out_specs=[block] * parts,
        ),
        out_shape=[jax.ShapeDtypeStruct(columns[0].shape, jnp.float32)] * parts,
        name=f"solve_columns_{group}",
    )(me, *columns, kernel, *ops)


def add_exchange(group, scalars, returned, flat, totals, tables):
    slots, planes, rows, lanes = flat.shape
    parts = len(returned)
    width = returned[0].shape[1]
    bx = BLOCK_PLANES

    def body(*refs):
        _, first, slot, weight, cross = refs[: len(scalars)]
        refs = refs[len(scalars):]
        data, refs = refs[:parts], refs[parts:]
        leads, seconds = refs[:GROUP], refs[GROUP : 2 * GROUP]
        yh, yl, zh, zl = refs[2 * GROUP : 2 * GROUP + 4]
        out = refs[-1]
        pieces = [data[d][c] for c in range(2) for d in range(parts)]
        turned = jnp.swapaxes(jnp.concatenate(pieces, axis=0), 0, 1)
        y = left(yh, yl, jnp.concatenate([turned[x] for x in range(bx)], axis=1))
        lines = [
            jnp.concatenate(
                [y[i * rows : (i + 1) * rows, x * lanes : (x + 1) * lanes] for i in range(4)],
                axis=1,
            )
            for x in range(bx)
        ]
        v = right_transposed(jnp.concatenate(lines, axis=0), zh, zl)
        if totals is None:
            out[...] = jnp.zeros_like(out)
        else:
            out[...] = refs[-2][...]
        for p in range(GROUP):
            at = group * GROUP + p
            potential = v[:, p * lanes : (p + 1) * lanes].reshape(bx, rows, lanes)
            out[first[at]] += weight[at] * potential * seconds[p][0]
            out[slot[at]] += cross[at] * potential * leads[p][0]

    ops = [*tables[4], *tables[0]]
    total_spec = pl.BlockSpec((slots, bx, rows, lanes), lambda i, *_: (0, i, 0, 0))
    in_specs = [pl.BlockSpec((2, width, bx, lanes), lambda i, *_: (0, 0, i, 0))] * parts
    in_specs += orbital_specs(group, bx, rows, lanes) + [table_spec(t) for t in ops]
    args = [*scalars, *returned, *([flat] * (2 * GROUP)), *ops]
    aliases = {}
    if totals is not None:
        in_specs.append(total_spec)
        aliases = {len(args): 0}
        args.append(totals)
    return pl.pallas_call(
        body,
        grid_spec=pltpu.PrefetchScalarGridSpec(
            num_scalar_prefetch=len(scalars),
            grid=(planes // bx,),
            in_specs=in_specs,
            out_specs=total_spec,
        ),
        out_shape=jax.ShapeDtypeStruct(flat.shape, jnp.float32),
        input_output_aliases=aliases,
        name=f"add_exchange_{group}",
    )(*args)


def live_pairs(pair_mask):
    pairs = pair_table()
    count = pairs.shape[0]
    slots = -(-CAP // GROUP) * GROUP
    band = lax.axis_index("band")
    groups = lax.axis_size("band")
    rows = band * ORB_DEV + jnp.asarray(pairs[:, 0])
    cols = (band + jnp.asarray(pairs[:, 1])) % groups * ORB_DEV + jnp.asarray(pairs[:, 2])
    live = pair_mask[rows, cols]
    earlier = np.tril(np.ones((count, count), np.int32), -1)
    rank = jnp.sum(jnp.asarray(earlier) * live[None, :], axis=1)
    hot = (rank[None, :] == jnp.arange(slots, dtype=jnp.int32)[:, None]) * live[None, :]
    slot_of = pairs[:, 1] * ORB_DEV + pairs[:, 2]
    cross_of = (slot_of != pairs[:, 0]).astype(np.int32)
    first = jnp.sum(hot * jnp.asarray(pairs[:, 0])[None, :], axis=1)
    slot = jnp.sum(hot * jnp.asarray(slot_of.astype(np.int32))[None, :], axis=1)
    weight = jnp.sum(hot, axis=1).astype(jnp.float32)
    cross = jnp.sum(hot * jnp.asarray(cross_of)[None, :], axis=1).astype(jnp.float32)
    return first, slot, weight, cross


def green_kernel(n, width):
    def wave(positions):
        return jnp.where(positions < n // 2, positions, positions - n)

    ky = wave(lax.axis_index("grid") * width + jnp.arange(width, dtype=jnp.int32))
    k = wave(jnp.arange(n, dtype=jnp.int32))
    kz = wave(jnp.arange(2 * n, dtype=jnp.int32) % n)
    squared = (ky * ky)[:, None, None] + (k * k)[None, :, None] + (kz * kz)[None, None, :]
    safe = jnp.maximum(squared, 1).astype(jnp.float32)
    scale = BOX_LENGTH * BOX_LENGTH / math.pi / float(n**3)
    return jnp.where(squared > 0, scale / safe, 0.0)


def local(orbitals, pair_mask):
    orb_count, planes, cells = orbitals.shape
    n = math.isqrt(cells)
    parts = lax.axis_size("grid")
    tables = dft_tables(n, parts)
    own = orbitals.reshape(orb_count, planes, n // 2, 2 * n)
    visits = [own] + [shifted(own, "band", -d) for d in range(1, REACH + 1)]
    flat = jnp.concatenate(visits, axis=0)
    me = lax.axis_index("grid").astype(jnp.int32).reshape(1)
    scalars = (me, *live_pairs(pair_mask))
    kernel = green_kernel(n, n // parts)

    order = peer_order(parts)

    def exchange(blocks):
        moved = [blocks[0]]
        for s in range(1, parts):
            back = order[order[0][s]].index(0)
            route = [(order[m][s], m) for m in range(parts)]
            moved.append(lax.ppermute(blocks[back], "grid", route))
        return moved

    turns = range(-(-CAP // GROUP))
    spectra = [forward_planes(g, scalars[:3], flat, tables, parts) for g in turns]
    columns = [exchange(s) for s in spectra]
    solved = [solve_columns(g, me, columns[g], kernel, tables) for g in turns]
    returned = [exchange(s) for s in solved]
    totals = None
    for g in turns:
        totals = add_exchange(g, scalars, returned[g], flat, totals, tables)
    owned = totals[:orb_count]
    for d in range(1, REACH + 1):
        owned = owned + shifted(totals[d * orb_count : (d + 1) * orb_count], "band", d)
    return (-MIXING * owned).reshape(orb_count, planes, cells)


def solution(mesh):
    return jax.shard_map(
        local,
        mesh=mesh,
        in_specs=(P("band", "grid", None), P()),
        out_specs=P("band", "grid", None),
        check_vma=False,
    )
```

```python
import math

import jax
import jax.numpy as jnp
import numpy as np
from jax import lax
from jax.experimental import pallas as pl
from jax.experimental.pallas import tpu as pltpu
from jax.sharding import PartitionSpec as P

ORB_DEV = 3
REACH = 2
CAP = 12
MIXING = 0.25
BOX_LENGTH = 16.0
GROUP = 4
BLOCK_PLANES = 8


def shifted(block, axis, distance):
    count = lax.axis_size(axis)
    return lax.ppermute(block, axis, [((i - distance) % count, i) for i in range(count)])


def pair_table():
    entries = []
    for distance in range(REACH + 1):
        for leading in range(ORB_DEV):
            for second in range(ORB_DEV):
                if distance > 0 or leading <= second:
                    entries.append((leading, distance, second))
    return np.array(entries, dtype=np.int32)


def split_table(table):
    high = table.astype(np.float32).astype(jnp.bfloat16)
    low = (table - high.astype(np.float64)).astype(np.float32).astype(jnp.bfloat16)
    return jnp.asarray(high), jnp.asarray(low)


def peer_order(parts):
    power = parts & (parts - 1) == 0
    return [[m ^ s if power else (m + s) % parts for s in range(parts)] for m in range(parts)]


def block_order(table, parts, side):
    n = table.shape[0] // 2
    stacked = []
    for order in peer_order(parts):
        index = np.arange(2 * n).reshape(2, parts, n // parts)[:, order].reshape(-1)
        stacked.append(table[index] if side == 0 else table[:, index])
    return np.stack(stacked)


def dft_tables(n, parts):
    k = np.arange(n)
    angles = (k[:, None] * k[None, :] % n) * (2.0 * math.pi / n)
    c, s = np.cos(angles), np.sin(angles)
    forward = np.array([[c, -s], [s, c]])
    inverse = np.array([[c, s], [-s, c]])
    e = np.eye(2)
    z_forward = np.einsum("cdzk,qr,yw->cqyzdwrk", forward, e, e).reshape(8 * n, 8 * n)
    f4 = forward.reshape(2, 2, n // 2, 2, n)
    y_forward = f4.transpose(1, 4, 0, 3, 2).reshape(2 * n, 2 * n)
    i4 = inverse.reshape(2, 2, n, n // 2, 2)
    y_inverse = i4.transpose(1, 4, 3, 0, 2).reshape(2 * n, 2 * n)
    x_forward = forward.transpose(1, 3, 0, 2).reshape(2 * n, 2 * n)
    x_inverse = inverse.transpose(1, 3, 0, 2).reshape(2 * n, 2 * n)
    y_forward = block_order(y_forward, parts, 0)
    x_forward = block_order(x_forward, parts, 1)
    x_inverse = block_order(x_inverse, parts, 0)
    y_inverse = block_order(y_inverse, parts, 1)
    named = (z_forward, y_forward, x_forward, x_inverse, y_inverse)
    return [split_table(t) for t in named]


def dot(a, b):
    return jnp.dot(a, b, preferred_element_type=jnp.float32)


def halves(x):
    high = x.astype(jnp.bfloat16)
    return high, (x - high.astype(jnp.float32)).astype(jnp.bfloat16)


def left(th, tl, x):
    xh, xl = halves(x)
    return dot(th[...], xh) + (dot(tl[...], xh) + dot(th[...], xl))


def right(x, th, tl):
    xh, xl = halves(x)
    return dot(xh, th[...]) + (dot(xh, tl[...]) + dot(xl, th[...]))


def right_transposed(x, th, tl):
    def dot_t(a, b):
        return lax.dot_general(a, b, (((1,), (1,)), ((), ())), preferred_element_type=jnp.float32)

    xh, xl = halves(x)
    return dot_t(xh, th[...]) + (dot_t(xh, tl[...]) + dot_t(xl, th[...]))


def table_spec(table):
    if table.ndim == 2:
        return pl.BlockSpec(table.shape, lambda *_: (0, 0))
    return pl.BlockSpec((pl.squeezed, *table.shape[1:]), lambda i, me, *_: (me[0], 0, 0))


def orbital_specs(group, bx, rows, lanes):
    def spec(which, p):
        return pl.BlockSpec(
            (1, bx, rows, lanes), lambda i, *s: (s[which + 1][group * GROUP + p], i, 0, 0)
        )

    return [spec(0, p) for p in range(GROUP)] + [spec(1, p) for p in range(GROUP)]


def forward_planes(group, half, scalars, flat, tables, parts):
    _, planes, rows, lanes = flat.shape
    n = lanes // 2
    width = n // parts
    bx = BLOCK_PLANES

    def body(*refs):
        refs = refs[len(scalars):]
        leads, seconds = refs[:GROUP], refs[GROUP : 2 * GROUP]
        zh, zl, yh, yl = refs[2 * GROUP : 2 * GROUP + 4]
        outs = refs[2 * GROUP + 4 :]
        rho = [(a[0] * b[0]).reshape(bx * rows, lanes) for a, b in zip(leads, seconds)]
        z = right(jnp.concatenate(rho, axis=1), zh, zl)
        cols = [
            jnp.concatenate(
                [z[x * rows : (x + 1) * rows, i * lanes : (i + 1) * lanes] for i in range(4)],
                axis=0,
            )
            for x in range(bx)
        ]
        y = left(yh, yl, jnp.concatenate(cols, axis=1))
        stacked = jnp.stack([y[:, x * lanes : (x + 1) * lanes] for x in range(bx)], axis=0)
        turned = jnp.swapaxes(stacked, 0, 1)
        for d in range(parts):
            for c in range(2):
                start = c * n + d * width
                outs[d][c] = turned[start : start + width]

    ops = [*tables[0], *tables[1]]
    return pl.pallas_call(
        body,
        grid_spec=pltpu.PrefetchScalarGridSpec(
            num_scalar_prefetch=len(scalars),
            grid=(planes // bx,),
            in_specs=orbital_specs(group, bx, rows, lanes) + [table_spec(t) for t in ops],
            out_specs=[pl.BlockSpec((2, width, bx, lanes), lambda i, *_: (0, 0, i, 0))] * parts,
        ),
        out_shape=[jax.ShapeDtypeStruct((2, width, planes, lanes), jnp.float32)] * parts,
        name=f"forward_planes_{group}_{half}",
    )(*scalars, *([flat] * (2 * GROUP)), *ops)


def solve_columns(group, me, columns, kernel, tables):
    pieces_each = len(columns[0])
    parts = len(columns)
    inputs = [piece for peer in columns for piece in peer]
    count = len(inputs)
    _, width, bx, lanes = inputs[0].shape
    planes = pieces_each * bx
    n = parts * planes
    bk = BLOCK_PLANES

    def body(_, *refs):
        data, outs = refs[:count], refs[count + 5 :]
        kern, fh, fl, ih, il = refs[count : count + 5]
        cols = []
        for k in range(bk):
            pieces = [data[d][c, k] for c in range(2) for d in range(count)]
            cols.append(jnp.concatenate(pieces, axis=0))
        spectrum = left(fh, fl, jnp.concatenate(cols, axis=1))
        weights = jnp.concatenate([kern[k] for k in range(bk)], axis=1)
        spectrum = spectrum * jnp.concatenate([weights, weights], axis=0)
        back = left(ih, il, spectrum)
        for k in range(bk):
            for c in range(2):
                for d in range(parts):
                    start = c * n + d * planes
                    outs[d][c, k] = back[start : start + planes, k * lanes : (k + 1) * lanes]

    ops = [*tables[2], *tables[3]]
    block = pl.BlockSpec((2, bk, planes, lanes), lambda i, *_: (0, i, 0, 0))
    return pl.pallas_call(
        body,
        grid_spec=pltpu.PrefetchScalarGridSpec(
            num_scalar_prefetch=1,
            grid=(width // bk,),
            in_specs=[pl.BlockSpec((2, bk, bx, lanes), lambda i, *_: (0, i, 0, 0))] * count
            + [pl.BlockSpec((bk, n, lanes), lambda i, *_: (i, 0, 0))]
            + [table_spec(t) for t in ops],
            out_specs=[block] * parts,
        ),
        out_shape=[jax.ShapeDtypeStruct((2, width, planes, lanes), jnp.float32)] * parts,
        name=f"solve_columns_{group}",
    )(me, *inputs, kernel, *ops)


def add_exchange(group, half, scalars, returned, flat, totals, tables):
    slots, planes, rows, lanes = flat.shape
    parts = len(returned)
    width = returned[0].shape[1]
    bx = BLOCK_PLANES

    def body(*refs):
        _, first, slot, weight, cross = refs[: len(scalars)]
        refs = refs[len(scalars):]
        data, refs = refs[:parts], refs[parts:]
        leads, seconds = refs[:GROUP], refs[GROUP : 2 * GROUP]
        yh, yl, zh, zl = refs[2 * GROUP : 2 * GROUP + 4]
        out = refs[-1]
        pieces = [data[d][c] for c in range(2) for d in range(parts)]
        turned = jnp.swapaxes(jnp.concatenate(pieces, axis=0), 0, 1)
        y = left(yh, yl, jnp.concatenate([turned[x] for x in range(bx)], axis=1))
        lines = [
            jnp.concatenate(
                [y[i * rows : (i + 1) * rows, x * lanes : (x + 1) * lanes] for i in range(4)],
                axis=1,
            )
            for x in range(bx)
        ]
        v = right_transposed(jnp.concatenate(lines, axis=0), zh, zl)
        if totals is None:
            out[...] = jnp.zeros_like(out)
        else:
            out[...] = refs[-2][...]
        for p in range(GROUP):
            at = group * GROUP + p
            potential = v[:, p * lanes : (p + 1) * lanes].reshape(bx, rows, lanes)
            out[first[at]] += weight[at] * potential * seconds[p][0]
            out[slot[at]] += cross[at] * potential * leads[p][0]

    ops = [*tables[4], *tables[0]]
    total_spec = pl.BlockSpec((slots, bx, rows, lanes), lambda i, *_: (0, i, 0, 0))
    in_specs = [pl.BlockSpec((2, width, bx, lanes), lambda i, *_: (0, 0, half, 0))] * parts
    in_specs += orbital_specs(group, bx, rows, lanes) + [table_spec(t) for t in ops]
    args = [*scalars, *returned, *([flat] * (2 * GROUP)), *ops]
    aliases = {}
    if totals is not None:
        in_specs.append(total_spec)
        aliases = {len(args): 0}
        args.append(totals)
    return pl.pallas_call(
        body,
        grid_spec=pltpu.PrefetchScalarGridSpec(
            num_scalar_prefetch=len(scalars),
            grid=(planes // bx,),
            in_specs=in_specs,
            out_specs=total_spec,
        ),
        out_shape=jax.ShapeDtypeStruct(flat.shape, jnp.float32),
        input_output_aliases=aliases,
        name=f"add_exchange_{group}_{half}",
    )(*args)


def live_pairs(pair_mask):
    pairs = pair_table()
    count = pairs.shape[0]
    slots = -(-CAP // GROUP) * GROUP
    band = lax.axis_index("band")
    groups = lax.axis_size("band")
    rows = band * ORB_DEV + jnp.asarray(pairs[:, 0])
    cols = (band + jnp.asarray(pairs[:, 1])) % groups * ORB_DEV + jnp.asarray(pairs[:, 2])
    live = pair_mask[rows, cols]
    earlier = np.tril(np.ones((count, count), np.int32), -1)
    rank = jnp.sum(jnp.asarray(earlier) * live[None, :], axis=1)
    hot = (rank[None, :] == jnp.arange(slots, dtype=jnp.int32)[:, None]) * live[None, :]
    slot_of = pairs[:, 1] * ORB_DEV + pairs[:, 2]
    cross_of = (slot_of != pairs[:, 0]).astype(np.int32)
    first = jnp.sum(hot * jnp.asarray(pairs[:, 0])[None, :], axis=1)
    slot = jnp.sum(hot * jnp.asarray(slot_of.astype(np.int32))[None, :], axis=1)
    weight = jnp.sum(hot, axis=1).astype(jnp.float32)
    cross = jnp.sum(hot * jnp.asarray(cross_of)[None, :], axis=1).astype(jnp.float32)
    return first, slot, weight, cross


def green_kernel(n, width):
    def wave(positions):
        return jnp.where(positions < n // 2, positions, positions - n)

    ky = wave(lax.axis_index("grid") * width + jnp.arange(width, dtype=jnp.int32))
    k = wave(jnp.arange(n, dtype=jnp.int32))
    kz = wave(jnp.arange(2 * n, dtype=jnp.int32) % n)
    squared = (ky * ky)[:, None, None] + (k * k)[None, :, None] + (kz * kz)[None, None, :]
    safe = jnp.maximum(squared, 1).astype(jnp.float32)
    scale = BOX_LENGTH * BOX_LENGTH / math.pi / float(n**3)
    return jnp.where(squared > 0, scale / safe, 0.0)


def pair_swap(block):
    return lax.ppermute(block, "band", [(i, i ^ 1) for i in range(lax.axis_size("band"))])


def visiting(own):
    if REACH != 2 or lax.axis_size("band") % 2:
        return [shifted(own, "band", -d) for d in range(1, REACH + 1)]
    even = lax.axis_index("band") % 2 == 0
    second = shifted(own, "band", -2)
    return [pair_swap(jnp.where(even, second, own)), second]


def collected(totals, count):
    pieces = [totals[d * count : (d + 1) * count] for d in range(REACH + 1)]
    if REACH != 2 or lax.axis_size("band") % 2:
        owned = pieces[0]
        for d in range(1, REACH + 1):
            owned = owned + shifted(pieces[d], "band", d)
        return owned
    even = lax.axis_index("band") % 2 == 0
    swapped = pair_swap(pieces[1])
    ahead = shifted(pieces[2] + jnp.where(even, swapped, 0.0), "band", 2)
    return pieces[0] + jnp.where(even, 0.0, swapped) + ahead


def local(orbitals, pair_mask):
    orb_count, planes, cells = orbitals.shape
    n = math.isqrt(cells)
    parts = lax.axis_size("grid")
    tables = dft_tables(n, parts)
    own = orbitals.reshape(orb_count, planes, n // 2, 2 * n)
    halves_of = range(planes // BLOCK_PLANES)
    flats = []
    for h in halves_of:
        mine = own[:, h * BLOCK_PLANES : (h + 1) * BLOCK_PLANES]
        flats.append(jnp.concatenate([mine, *visiting(mine)], axis=0))
    me = lax.axis_index("grid").astype(jnp.int32).reshape(1)
    scalars = (me, *live_pairs(pair_mask))
    kernel = green_kernel(n, n // parts)

    order = peer_order(parts)

    def exchange(blocks):
        moved = [blocks[0]]
        for s in range(1, parts):
            back = order[order[0][s]].index(0)
            route = [(order[m][s], m) for m in range(parts)]
            moved.append(lax.ppermute(blocks[back], "grid", route))
        return moved

    turns = range(-(-CAP // GROUP))
    moved = [
        [exchange(forward_planes(g, h, scalars[:3], flats[h], tables, parts)) for g in turns]
        for h in halves_of
    ]
    returned = []
    for g in turns:
        columns = [[moved[h][g][s] for h in halves_of] for s in range(parts)]
        returned.append(exchange(solve_columns(g, me, columns, kernel, tables)))
    owned = []
    for h in halves_of:
        totals = None
        for g in turns:
            totals = add_exchange(g, h, scalars, returned[g], flats[h], totals, tables)
        owned.append(collected(totals, orb_count))
    total = jnp.concatenate(owned, axis=1)
    return (-MIXING * total).reshape(orb_count, planes, cells)


def solution(mesh):
    return jax.shard_map(
        local,
        mesh=mesh,
        in_specs=(P("band", "grid", None), P()),
        out_specs=P("band", "grid", None),
        check_vma=False,
    )
```

```python
import math

import jax
import jax.numpy as jnp
import numpy as np
from jax import lax
from jax.experimental import pallas as pl
from jax.experimental.pallas import tpu as pltpu
from jax.sharding import PartitionSpec as P

ORB_DEV = 3
REACH = 2
CAP = 12
MIXING = 0.25
BOX_LENGTH = 16.0
GROUP = 4
BLOCK_PLANES = 8


def shifted(block, axis, distance):
    count = lax.axis_size(axis)
    return lax.ppermute(block, axis, [((i - distance) % count, i) for i in range(count)])


def pair_table():
    entries = []
    for distance in range(REACH + 1):
        for leading in range(ORB_DEV):
            for second in range(ORB_DEV):
                if distance > 0 or leading <= second:
                    entries.append((leading, distance, second))
    return np.array(entries, dtype=np.int32)


def split_table(table):
    high = table.astype(np.float32).astype(jnp.bfloat16)
    low = (table - high.astype(np.float64)).astype(np.float32).astype(jnp.bfloat16)
    return jnp.asarray(high), jnp.asarray(low)


def peer_order(parts):
    power = parts & (parts - 1) == 0
    return [[m ^ s if power else (m + s) % parts for s in range(parts)] for m in range(parts)]


def block_order(table, parts, side):
    n = table.shape[0] // 2
    stacked = []
    for order in peer_order(parts):
        index = np.arange(2 * n).reshape(2, parts, n // parts)[:, order].reshape(-1)
        stacked.append(table[index] if side == 0 else table[:, index])
    return np.stack(stacked)


def dft_tables(n, parts):
    k = np.arange(n)
    angles = (k[:, None] * k[None, :] % n) * (2.0 * math.pi / n)
    c, s = np.cos(angles), np.sin(angles)
    forward = np.array([[c, -s], [s, c]])
    inverse = np.array([[c, s], [-s, c]])
    e = np.eye(2)
    z_forward = np.einsum("cdzk,qr,yw->cqyzdwrk", forward, e, e).reshape(8 * n, 8 * n)
    f4 = forward.reshape(2, 2, n // 2, 2, n)
    y_forward = f4.transpose(1, 4, 0, 3, 2).reshape(2 * n, 2 * n)
    i4 = inverse.reshape(2, 2, n, n // 2, 2)
    y_inverse = i4.transpose(1, 4, 3, 0, 2).reshape(2 * n, 2 * n)
    x_forward = forward.transpose(1, 3, 0, 2).reshape(2 * n, 2 * n)
    x_inverse = inverse.transpose(1, 3, 0, 2).reshape(2 * n, 2 * n)
    y_forward = block_order(y_forward, parts, 0)
    x_forward = block_order(x_forward, parts, 1)
    x_inverse = block_order(x_inverse, parts, 0)
    y_inverse = block_order(y_inverse, parts, 1)
    named = (z_forward, y_forward, x_forward, x_inverse, y_inverse)
    return [split_table(t) for t in named]


def dot(a, b):
    return jnp.dot(a, b, preferred_element_type=jnp.float32)


def halves(x):
    high = x.astype(jnp.bfloat16)
    return high, (x - high.astype(jnp.float32)).astype(jnp.bfloat16)


def left(th, tl, x):
    xh, xl = halves(x)
    return dot(th[...], xh) + (dot(tl[...], xh) + dot(th[...], xl))


def right(x, th, tl):
    xh, xl = halves(x)
    return dot(xh, th[...]) + (dot(xh, tl[...]) + dot(xl, th[...]))


def right_transposed(x, th, tl):
    def dot_t(a, b):
        return lax.dot_general(a, b, (((1,), (1,)), ((), ())), preferred_element_type=jnp.float32)

    xh, xl = halves(x)
    return dot_t(xh, th[...]) + (dot_t(xh, tl[...]) + dot_t(xl, th[...]))


def table_spec(table):
    if table.ndim == 2:
        return pl.BlockSpec(table.shape, lambda *_: (0, 0))
    return pl.BlockSpec((pl.squeezed, *table.shape[1:]), lambda i, me, *_: (me[0], 0, 0))


def orbital_specs(group, bx, rows, lanes):
    def spec(which, p):
        return pl.BlockSpec(
            (1, bx, rows, lanes), lambda i, *s: (s[which + 1][group * GROUP + p], i, 0, 0)
        )

    return [spec(0, p) for p in range(GROUP)] + [spec(1, p) for p in range(GROUP)]


def forward_planes(group, scalars, flat, tables, parts):
    _, planes, rows, lanes = flat.shape
    n = lanes // 2
    width = n // parts
    bx = BLOCK_PLANES

    def body(*refs):
        refs = refs[len(scalars):]
        leads, seconds = refs[:GROUP], refs[GROUP : 2 * GROUP]
        zh, zl, yh, yl = refs[2 * GROUP : 2 * GROUP + 4]
        outs = refs[2 * GROUP + 4 :]
        rho = [(a[0] * b[0]).reshape(bx * rows, lanes) for a, b in zip(leads, seconds)]
        z = right(jnp.concatenate(rho, axis=1), zh, zl)
        cols = [
            jnp.concatenate(
                [z[x * rows : (x + 1) * rows, i * lanes : (i + 1) * lanes] for i in range(4)],
                axis=0,
            )
            for x in range(bx)
        ]
        y = left(yh, yl, jnp.concatenate(cols, axis=1))
        stacked = jnp.stack([y[:, x * lanes : (x + 1) * lanes] for x in range(bx)], axis=0)
        turned = jnp.swapaxes(stacked, 0, 1)
        for d in range(parts):
            for c in range(2):
                start = c * n + d * width
                outs[d][c] = turned[start : start + width]

    ops = [*tables[0], *tables[1]]
    return pl.pallas_call(
        body,
        grid_spec=pltpu.PrefetchScalarGridSpec(
            num_scalar_prefetch=len(scalars),
            grid=(planes // bx,),
            in_specs=orbital_specs(group, bx, rows, lanes) + [table_spec(t) for t in ops],
            out_specs=[pl.BlockSpec((2, width, bx, lanes), lambda i, *_: (0, 0, i, 0))] * parts,
        ),
        out_shape=[jax.ShapeDtypeStruct((2, width, planes, lanes), jnp.float32)] * parts,
        name=f"forward_planes_{group}",
    )(*scalars, *([flat] * (2 * GROUP)), *ops)


def solve_columns(group, me, columns, kernel, tables):
    parts = len(columns)
    _, width, planes, lanes = columns[0].shape
    n = parts * planes
    bk = BLOCK_PLANES

    def body(_, *refs):
        data, outs = refs[:parts], refs[parts + 5 :]
        kern, fh, fl, ih, il = refs[parts : parts + 5]
        cols = []
        for k in range(bk):
            pieces = [data[d][c, k] for c in range(2) for d in range(parts)]
            cols.append(jnp.concatenate(pieces, axis=0))
        spectrum = left(fh, fl, jnp.concatenate(cols, axis=1))
        weights = jnp.concatenate([kern[k] for k in range(bk)], axis=1)
        spectrum = spectrum * jnp.concatenate([weights, weights], axis=0)
        back = left(ih, il, spectrum)
        for k in range(bk):
            for c in range(2):
                for d in range(parts):
                    start = c * n + d * planes
                    outs[d][c, k] = back[start : start + planes, k * lanes : (k + 1) * lanes]

    ops = [*tables[2], *tables[3]]
    block = pl.BlockSpec((2, bk, planes, lanes), lambda i, *_: (0, i, 0, 0))
    return pl.pallas_call(
        body,
        grid_spec=pltpu.PrefetchScalarGridSpec(
            num_scalar_prefetch=1,
            grid=(width // bk,),
            in_specs=[block] * parts
            + [pl.BlockSpec((bk, n, lanes), lambda i, *_: (i, 0, 0))]
            + [table_spec(t) for t in ops],
            out_specs=[block] * parts,
        ),
        out_shape=[jax.ShapeDtypeStruct(columns[0].shape, jnp.float32)] * parts,
        name=f"solve_columns_{group}",
    )(me, *columns, kernel, *ops)


def add_exchange(group, scalars, returned, flat, totals, tables):
    slots, planes, rows, lanes = flat.shape
    parts = len(returned)
    width = returned[0].shape[1]
    bx = BLOCK_PLANES

    def body(*refs):
        _, first, slot, weight, cross = refs[: len(scalars)]
        refs = refs[len(scalars):]
        data, refs = refs[:parts], refs[parts:]
        leads, seconds = refs[:GROUP], refs[GROUP : 2 * GROUP]
        yh, yl, zh, zl = refs[2 * GROUP : 2 * GROUP + 4]
        out = refs[-1]
        pieces = [data[d][c] for c in range(2) for d in range(parts)]
        turned = jnp.swapaxes(jnp.concatenate(pieces, axis=0), 0, 1)
        y = left(yh, yl, jnp.concatenate([turned[x] for x in range(bx)], axis=1))
        lines = [
            jnp.concatenate(
                [y[i * rows : (i + 1) * rows, x * lanes : (x + 1) * lanes] for i in range(4)],
                axis=1,
            )
            for x in range(bx)
        ]
        v = right_transposed(jnp.concatenate(lines, axis=0), zh, zl)
        if totals is None:
            out[...] = jnp.zeros_like(out)
        else:
            out[...] = refs[-2][...]
        for p in range(GROUP):
            at = group * GROUP + p
            potential = v[:, p * lanes : (p + 1) * lanes].reshape(bx, rows, lanes)
            out[first[at]] += weight[at] * potential * seconds[p][0]
            out[slot[at]] += cross[at] * potential * leads[p][0]

    ops = [*tables[4], *tables[0]]
    total_spec = pl.BlockSpec((slots, bx, rows, lanes), lambda i, *_: (0, i, 0, 0))
    in_specs = [pl.BlockSpec((2, width, bx, lanes), lambda i, *_: (0, 0, i, 0))] * parts
    in_specs += orbital_specs(group, bx, rows, lanes) + [table_spec(t) for t in ops]
    args = [*scalars, *returned, *([flat] * (2 * GROUP)), *ops]
    aliases = {}
    if totals is not None:
        in_specs.append(total_spec)
        aliases = {len(args): 0}
        args.append(totals)
    return pl.pallas_call(
        body,
        grid_spec=pltpu.PrefetchScalarGridSpec(
            num_scalar_prefetch=len(scalars),
            grid=(planes // bx,),
            in_specs=in_specs,
            out_specs=total_spec,
        ),
        out_shape=jax.ShapeDtypeStruct(flat.shape, jnp.float32),
        input_output_aliases=aliases,
        name=f"add_exchange_{group}",
    )(*args)


def live_pairs(pair_mask):
    pairs = pair_table()
    count = pairs.shape[0]
    slots = -(-CAP // GROUP) * GROUP
    band = lax.axis_index("band")
    groups = lax.axis_size("band")
    rows = band * ORB_DEV + jnp.asarray(pairs[:, 0])
    cols = (band + jnp.asarray(pairs[:, 1])) % groups * ORB_DEV + jnp.asarray(pairs[:, 2])
    live = pair_mask[rows, cols]
    earlier = np.tril(np.ones((count, count), np.int32), -1)
    rank = jnp.sum(jnp.asarray(earlier) * live[None, :], axis=1)
    hot = (rank[None, :] == jnp.arange(slots, dtype=jnp.int32)[:, None]) * live[None, :]
    slot_of = pairs[:, 1] * ORB_DEV + pairs[:, 2]
    cross_of = (slot_of != pairs[:, 0]).astype(np.int32)
    first = jnp.sum(hot * jnp.asarray(pairs[:, 0])[None, :], axis=1)
    slot = jnp.sum(hot * jnp.asarray(slot_of.astype(np.int32))[None, :], axis=1)
    weight = jnp.sum(hot, axis=1).astype(jnp.float32)
    cross = jnp.sum(hot * jnp.asarray(cross_of)[None, :], axis=1).astype(jnp.float32)
    return first, slot, weight, cross


def green_kernel(n, width):
    def wave(positions):
        return jnp.where(positions < n // 2, positions, positions - n)

    ky = wave(lax.axis_index("grid") * width + jnp.arange(width, dtype=jnp.int32))
    k = wave(jnp.arange(n, dtype=jnp.int32))
    kz = wave(jnp.arange(2 * n, dtype=jnp.int32) % n)
    squared = (ky * ky)[:, None, None] + (k * k)[None, :, None] + (kz * kz)[None, None, :]
    safe = jnp.maximum(squared, 1).astype(jnp.float32)
    scale = BOX_LENGTH * BOX_LENGTH / math.pi / float(n**3)
    return jnp.where(squared > 0, scale / safe, 0.0)


def pair_swap(block):
    return lax.ppermute(block, "band", [(i, i ^ 1) for i in range(lax.axis_size("band"))])


def visiting(own):
    if REACH != 2 or lax.axis_size("band") % 2:
        return [shifted(own, "band", -d) for d in range(1, REACH + 1)]
    even = lax.axis_index("band") % 2 == 0
    second = shifted(own, "band", -2)
    return [pair_swap(jnp.where(even, second, own)), second]


def collected(totals, at):
    pieces = [totals[d * ORB_DEV + at : d * ORB_DEV + at + 1] for d in range(REACH + 1)]
    if REACH != 2 or lax.axis_size("band") % 2:
        owned = pieces[0]
        for d in range(1, REACH + 1):
            owned = owned + shifted(pieces[d], "band", d)
        return owned
    even = lax.axis_index("band") % 2 == 0
    swapped = pair_swap(pieces[1])
    ahead = shifted(pieces[2] + jnp.where(even, swapped, 0.0), "band", 2)
    return pieces[0] + jnp.where(even, 0.0, swapped) + ahead


def local(orbitals, pair_mask):
    orb_count, planes, cells = orbitals.shape
    n = math.isqrt(cells)
    parts = lax.axis_size("grid")
    tables = dft_tables(n, parts)
    own = orbitals.reshape(orb_count, planes, n // 2, 2 * n)
    visits = [visiting(own[a : a + 1]) for a in range(orb_count)]
    flat = jnp.concatenate([own] + [v[d] for d in range(REACH) for v in visits], axis=0)
    me = lax.axis_index("grid").astype(jnp.int32).reshape(1)
    scalars = (me, *live_pairs(pair_mask))
    kernel = green_kernel(n, n // parts)

    order = peer_order(parts)

    def exchange(blocks):
        moved = [blocks[0]]
        for s in range(1, parts):
            back = order[order[0][s]].index(0)
            route = [(order[m][s], m) for m in range(parts)]
            moved.append(lax.ppermute(blocks[back], "grid", route))
        return moved

    turns = range(-(-CAP // GROUP))
    spectra = [forward_planes(g, scalars[:3], flat, tables, parts) for g in turns]
    columns = [exchange(s) for s in spectra]
    solved = [solve_columns(g, me, columns[g], kernel, tables) for g in turns]
    returned = [exchange(s) for s in solved]
    totals = None
    for g in turns:
        totals = add_exchange(g, scalars, returned[g], flat, totals, tables)
    owned = jnp.concatenate([collected(totals, a) for a in range(orb_count)], axis=0)
    return (-MIXING * owned).reshape(orb_count, planes, cells)


def solution(mesh):
    return jax.shard_map(
        local,
        mesh=mesh,
        in_specs=(P("band", "grid", None), P()),
        out_specs=P("band", "grid", None),
        check_vma=False,
    )
```

```python
import math

import jax
import jax.numpy as jnp
import numpy as np
from jax import lax
from jax.experimental import pallas as pl
from jax.experimental.pallas import tpu as pltpu
from jax.sharding import PartitionSpec as P

ORB_DEV = 3
REACH = 2
CAP = 12
MIXING = 0.25
BOX_LENGTH = 16.0
GROUP = 4
BLOCK_PLANES = 8


def shifted(block, axis, distance):
    count = lax.axis_size(axis)
    return lax.ppermute(block, axis, [((i - distance) % count, i) for i in range(count)])


def pair_table():
    entries = []
    for distance in range(REACH + 1):
        for leading in range(ORB_DEV):
            for second in range(ORB_DEV):
                if distance > 0 or leading <= second:
                    entries.append((leading, distance, second))
    return np.array(entries, dtype=np.int32)


def split_table(table):
    high = table.astype(np.float32).astype(jnp.bfloat16)
    low = (table - high.astype(np.float64)).astype(np.float32).astype(jnp.bfloat16)
    return jnp.asarray(high), jnp.asarray(low)


def peer_order(parts):
    power = parts & (parts - 1) == 0
    return [[m ^ s if power else (m + s) % parts for s in range(parts)] for m in range(parts)]


def block_order(table, parts, side):
    n = table.shape[0] // 2
    stacked = []
    for order in peer_order(parts):
        index = np.arange(2 * n).reshape(2, parts, n // parts)[:, order].reshape(-1)
        stacked.append(table[index] if side == 0 else table[:, index])
    return np.stack(stacked)


def dft_tables(n, parts):
    k = np.arange(n)
    angles = (k[:, None] * k[None, :] % n) * (2.0 * math.pi / n)
    c, s = np.cos(angles), np.sin(angles)
    forward = np.array([[c, -s], [s, c]])
    inverse = np.array([[c, s], [-s, c]])
    e = np.eye(2)
    z_forward = np.einsum("cdzk,qr,yw->cqyzdwrk", forward, e, e).reshape(8 * n, 8 * n)
    f4 = forward.reshape(2, 2, n // 2, 2, n)
    y_forward = f4.transpose(1, 4, 0, 3, 2).reshape(2 * n, 2 * n)
    i4 = inverse.reshape(2, 2, n, n // 2, 2)
    y_inverse = i4.transpose(1, 4, 3, 0, 2).reshape(2 * n, 2 * n)
    x_forward = forward.transpose(1, 3, 0, 2).reshape(2 * n, 2 * n)
    x_inverse = inverse.transpose(1, 3, 0, 2).reshape(2 * n, 2 * n)
    y_forward = block_order(y_forward, parts, 0)
    x_forward = block_order(x_forward, parts, 1)
    x_inverse = block_order(x_inverse, parts, 0)
    y_inverse = block_order(y_inverse, parts, 1)
    named = (z_forward, y_forward, x_forward, x_inverse, y_inverse)
    return [split_table(t) for t in named]


def dot(a, b):
    return jnp.dot(a, b, preferred_element_type=jnp.float32)


def halves(x):
    high = x.astype(jnp.bfloat16)
    return high, (x - high.astype(jnp.float32)).astype(jnp.bfloat16)


def left(th, tl, x):
    xh, xl = halves(x)
    return dot(th[...], xh) + (dot(tl[...], xh) + dot(th[...], xl))


def right(x, th, tl):
    xh, xl = halves(x)
    return dot(xh, th[...]) + (dot(xh, tl[...]) + dot(xl, th[...]))


def right_transposed(x, th, tl):
    def dot_t(a, b):
        return lax.dot_general(a, b, (((1,), (1,)), ((), ())), preferred_element_type=jnp.float32)

    xh, xl = halves(x)
    return dot_t(xh, th[...]) + (dot_t(xh, tl[...]) + dot_t(xl, th[...]))


def table_spec(table):
    if table.ndim == 2:
        return pl.BlockSpec(table.shape, lambda *_: (0, 0))
    return pl.BlockSpec((pl.squeezed, *table.shape[1:]), lambda i, me, *_: (me[0], 0, 0))


def orbital_specs(group, bx, rows, lanes):
    def spec(which, p):
        return pl.BlockSpec(
            (1, bx, rows, lanes), lambda i, *s: (s[which + 1][group * GROUP + p], i, 0, 0)
        )

    return [spec(0, p) for p in range(GROUP)] + [spec(1, p) for p in range(GROUP)]


def forward_planes(group, scalars, flat, tables, parts):
    _, planes, rows, lanes = flat.shape
    n = lanes // 2
    width = n // parts
    bx = BLOCK_PLANES

    def body(*refs):
        refs = refs[len(scalars):]
        leads, seconds = refs[:GROUP], refs[GROUP : 2 * GROUP]
        zh, zl, yh, yl = refs[2 * GROUP : 2 * GROUP + 4]
        outs = refs[2 * GROUP + 4 :]
        rho = [(a[0] * b[0]).reshape(bx * rows, lanes) for a, b in zip(leads, seconds)]
        z = right(jnp.concatenate(rho, axis=1), zh, zl)
        cols = [
            jnp.concatenate(
                [z[x * rows : (x + 1) * rows, i * lanes : (i + 1) * lanes] for i in range(4)],
                axis=0,
            )
            for x in range(bx)
        ]
        y = left(yh, yl, jnp.concatenate(cols, axis=1))
        stacked = jnp.stack([y[:, x * lanes : (x + 1) * lanes] for x in range(bx)], axis=0)
        turned = jnp.swapaxes(stacked, 0, 1)
        for d in range(parts):
            for c in range(2):
                start = c * n + d * width
                outs[d][c] = turned[start : start + width]

    ops = [*tables[0], *tables[1]]
    return pl.pallas_call(
        body,
        grid_spec=pltpu.PrefetchScalarGridSpec(
            num_scalar_prefetch=len(scalars),
            grid=(planes // bx,),
            in_specs=orbital_specs(group, bx, rows, lanes) + [table_spec(t) for t in ops],
            out_specs=[pl.BlockSpec((2, width, bx, lanes), lambda i, *_: (0, 0, i, 0))] * parts,
        ),
        out_shape=[jax.ShapeDtypeStruct((2, width, planes, lanes), jnp.float32)] * parts,
        name=f"forward_planes_{group}",
    )(*scalars, *([flat] * (2 * GROUP)), *ops)


def solve_columns(group, me, columns, kernel, tables):
    parts = len(columns)
    _, width, planes, lanes = columns[0].shape
    n = parts * planes
    bk = BLOCK_PLANES

    def body(_, *refs):
        data, outs = refs[:parts], refs[parts + 5 :]
        kern, fh, fl, ih, il = refs[parts : parts + 5]
        cols = []
        for k in range(bk):
            pieces = [data[d][c, k] for c in range(2) for d in range(parts)]
            cols.append(jnp.concatenate(pieces, axis=0))
        spectrum = left(fh, fl, jnp.concatenate(cols, axis=1))
        weights = jnp.concatenate([kern[k] for k in range(bk)], axis=1)
        spectrum = spectrum * jnp.concatenate([weights, weights], axis=0)
        back = left(ih, il, spectrum)
        for k in range(bk):
            for c in range(2):
                for d in range(parts):
                    start = c * n + d * planes
                    outs[d][c, k] = back[start : start + planes, k * lanes : (k + 1) * lanes]

    ops = [*tables[2], *tables[3]]
    block = pl.BlockSpec((2, bk, planes, lanes), lambda i, *_: (0, i, 0, 0))
    return pl.pallas_call(
        body,
        grid_spec=pltpu.PrefetchScalarGridSpec(
            num_scalar_prefetch=1,
            grid=(width // bk,),
            in_specs=[block] * parts
            + [pl.BlockSpec((bk, n, lanes), lambda i, *_: (i, 0, 0))]
            + [table_spec(t) for t in ops],
            out_specs=[block] * parts,
        ),
        out_shape=[jax.ShapeDtypeStruct(columns[0].shape, jnp.float32)] * parts,
        name=f"solve_columns_{group}",
    )(me, *columns, kernel, *ops)


def add_exchange(group, scalars, returned, flat, totals, tables):
    slots, planes, rows, lanes = flat.shape
    parts = len(returned)
    width = returned[0].shape[1]
    bx = BLOCK_PLANES

    def body(*refs):
        _, first, slot, weight, cross = refs[: len(scalars)]
        refs = refs[len(scalars):]
        data, refs = refs[:parts], refs[parts:]
        leads, seconds = refs[:GROUP], refs[GROUP : 2 * GROUP]
        yh, yl, zh, zl = refs[2 * GROUP : 2 * GROUP + 4]
        out = refs[-1]
        pieces = [data[d][c] for c in range(2) for d in range(parts)]
        turned = jnp.swapaxes(jnp.concatenate(pieces, axis=0), 0, 1)
        y = left(yh, yl, jnp.concatenate([turned[x] for x in range(bx)], axis=1))
        lines = [
            jnp.concatenate(
                [y[i * rows : (i + 1) * rows, x * lanes : (x + 1) * lanes] for i in range(4)],
                axis=1,
            )
            for x in range(bx)
        ]
        v = right_transposed(jnp.concatenate(lines, axis=0), zh, zl)
        if totals is None:
            out[...] = jnp.zeros_like(out)
        else:
            out[...] = refs[-2][...]
        for p in range(GROUP):
            at = group * GROUP + p
            potential = v[:, p * lanes : (p + 1) * lanes].reshape(bx, rows, lanes)
            out[first[at]] += weight[at] * potential * seconds[p][0]
            out[slot[at]] += cross[at] * potential * leads[p][0]

    ops = [*tables[4], *tables[0]]
    total_spec = pl.BlockSpec((slots, bx, rows, lanes), lambda i, *_: (0, i, 0, 0))
    in_specs = [pl.BlockSpec((2, width, bx, lanes), lambda i, *_: (0, 0, i, 0))] * parts
    in_specs += orbital_specs(group, bx, rows, lanes) + [table_spec(t) for t in ops]
    args = [*scalars, *returned, *([flat] * (2 * GROUP)), *ops]
    aliases = {}
    if totals is not None:
        in_specs.append(total_spec)
        aliases = {len(args): 0}
        args.append(totals)
    return pl.pallas_call(
        body,
        grid_spec=pltpu.PrefetchScalarGridSpec(
            num_scalar_prefetch=len(scalars),
            grid=(planes // bx,),
            in_specs=in_specs,
            out_specs=total_spec,
        ),
        out_shape=jax.ShapeDtypeStruct(flat.shape, jnp.float32),
        input_output_aliases=aliases,
        name=f"add_exchange_{group}",
    )(*args)


def live_pairs(pair_mask):
    pairs = pair_table()
    count = pairs.shape[0]
    slots = -(-CAP // GROUP) * GROUP
    band = lax.axis_index("band")
    groups = lax.axis_size("band")
    rows = band * ORB_DEV + jnp.asarray(pairs[:, 0])
    cols = (band + jnp.asarray(pairs[:, 1])) % groups * ORB_DEV + jnp.asarray(pairs[:, 2])
    live = pair_mask[rows, cols]
    earlier = np.tril(np.ones((count, count), np.int32), -1)
    rank = jnp.sum(jnp.asarray(earlier) * live[None, :], axis=1)
    hot = (rank[None, :] == jnp.arange(slots, dtype=jnp.int32)[:, None]) * live[None, :]
    slot_of = pairs[:, 1] * ORB_DEV + pairs[:, 2]
    cross_of = (slot_of != pairs[:, 0]).astype(np.int32)
    first = jnp.sum(hot * jnp.asarray(pairs[:, 0])[None, :], axis=1)
    slot = jnp.sum(hot * jnp.asarray(slot_of.astype(np.int32))[None, :], axis=1)
    weight = jnp.sum(hot, axis=1).astype(jnp.float32)
    cross = jnp.sum(hot * jnp.asarray(cross_of)[None, :], axis=1).astype(jnp.float32)
    return first, slot, weight, cross


def green_kernel(n, width):
    def wave(positions):
        return jnp.where(positions < n // 2, positions, positions - n)

    ky = wave(lax.axis_index("grid") * width + jnp.arange(width, dtype=jnp.int32))
    k = wave(jnp.arange(n, dtype=jnp.int32))
    kz = wave(jnp.arange(2 * n, dtype=jnp.int32) % n)
    squared = (ky * ky)[:, None, None] + (k * k)[None, :, None] + (kz * kz)[None, None, :]
    safe = jnp.maximum(squared, 1).astype(jnp.float32)
    scale = BOX_LENGTH * BOX_LENGTH / math.pi / float(n**3)
    return jnp.where(squared > 0, scale / safe, 0.0)


def pair_swap(block):
    return lax.ppermute(block, "band", [(i, i ^ 1) for i in range(lax.axis_size("band"))])


def visiting(own):
    if REACH != 2 or lax.axis_size("band") % 2:
        return [shifted(own, "band", -d) for d in range(1, REACH + 1)]
    even = lax.axis_index("band") % 2 == 0
    second = shifted(own, "band", -2)
    return [pair_swap(jnp.where(even, second, own)), second]


def local(orbitals, pair_mask):
    orb_count, planes, cells = orbitals.shape
    n = math.isqrt(cells)
    parts = lax.axis_size("grid")
    tables = dft_tables(n, parts)
    own = orbitals.reshape(orb_count, planes, n // 2, 2 * n)
    visits = [visiting(own[a : a + 1]) for a in range(orb_count)]
    flat = jnp.concatenate([own] + [v[d] for d in range(REACH) for v in visits], axis=0)
    me = lax.axis_index("grid").astype(jnp.int32).reshape(1)
    scalars = (me, *live_pairs(pair_mask))
    kernel = green_kernel(n, n // parts)

    order = peer_order(parts)

    def exchange(blocks):
        moved = [blocks[0]]
        for s in range(1, parts):
            back = order[order[0][s]].index(0)
            route = [(order[m][s], m) for m in range(parts)]
            moved.append(lax.ppermute(blocks[back], "grid", route))
        return moved

    turns = range(-(-CAP // GROUP))
    spectra = [forward_planes(g, scalars[:3], flat, tables, parts) for g in turns]
    columns = [exchange(s) for s in spectra]
    solved = [solve_columns(g, me, columns[g], kernel, tables) for g in turns]
    returned = [exchange(s) for s in solved]
    totals = None
    for g in turns:
        totals = add_exchange(g, scalars, returned[g], flat, totals, tables)
    owned = totals[:orb_count]
    for d in range(1, REACH + 1):
        owned = owned + shifted(totals[d * orb_count : (d + 1) * orb_count], "band", d)
    return (-MIXING * owned).reshape(orb_count, planes, cells)


def solution(mesh):
    return jax.shard_map(
        local,
        mesh=mesh,
        in_specs=(P("band", "grid", None), P()),
        out_specs=P("band", "grid", None),
        check_vma=False,
    )
```
